128 devices in a mesh: row: 16 (over x, y), col: 8 (over z, core).
Axes of the slice: x: 4, y: 4, z: 4, core: 2. Of those that a mesh axis runs over, the one named last changes fastest.
Arguments:
- matrix: float32 [32768, 8192], P('row', 'col'), may hold values from -40 to 40
Outputs:
- upper: float32 [256, 8192], P('row', 'col')
- reduced: float32 [32768, 8192], P('row', 'col')
The draws below stay inside these ranges and needn't reach their ends.
All inputs are finite; a program needn't handle non-finite values.
Results may differ from the reference program's by a relative error of at most 0.0003.
Values sent between devices are 32-bit elements; how exact they have to be, the bound alone decides.
No kernel may reach another device: no remote copies, remote signals or barrier semaphores. Data moves between devices by JAX's collectives and lax.ppermute only.
A program may use at most 128 MiB of HBM per device.

```python
import jax
import jax.numpy as jnp
from jax import lax

COLS = 8192
PANEL = 256
ROWS = 32768


def draw_matrix(key, part):
    base = jax.random.normal(jax.random.fold_in(key, 1), (ROWS, COLS), jnp.float32)
    return jnp.clip(base, -40.0, 40.0)


def setup_inputs(seed: int = 0) -> dict:
    key_list = jax.random.split(jax.random.key(seed), 2)
    return {
        "matrix": draw_matrix(jax.random.fold_in(key_list[1], 71), 0),
    }


def reference(matrix):
    panel = matrix[:, :PANEL]
    basis, factor = jnp.linalg.qr(panel)
    signs = jnp.sign(jnp.diagonal(factor))
    basis = basis * signs[None, :]
    upper = jnp.dot(basis.T.astype(jnp.float32), matrix.astype(jnp.float32), precision=lax.Precision.HIGHEST, preferred_element_type=jnp.float32)
    rest = matrix[:, PANEL:] - jnp.dot(basis.astype(jnp.float32), upper[:, PANEL:].astype(jnp.float32), precision=lax.Precision.HIGHEST, preferred_element_type=jnp.float32)
    scale = jnp.sqrt(jnp.float32(ROWS))
    reduced = jnp.concatenate([basis * scale, rest], axis=1)
    return (upper, reduced)
```

```python
import jax
import jax.numpy as jnp
from jax import lax
from jax.sharding import Mesh
from jax.sharding import PartitionSpec as P

PANEL = 256
COL = ("z", "c")
EXACT = lax.Precision.HIGHEST
HIGH = lax.Precision.HIGH


def dot(left, right, contract, precision):
    return lax.dot_general(
        left, right, (contract, ((), ())), precision=precision, preferred_element_type=jnp.float32
    )


def from_everyone(shard, axis):
    copies = jnp.broadcast_to(shard, (lax.axis_size(axis), *shard.shape))
    return lax.all_to_all(copies, axis, 0, 0, tiled=True)


def spread_panel(panel, col):
    half = panel.shape[0] // 2
    low, high = panel[:half], panel[half:]
    first = col == 0
    low = jnp.where(first, low, 0.0)
    high = jnp.where(first, high, 0.0)
    low = low + lax.ppermute(low, COL, [(0, 2)])
    high = high + lax.ppermute(high, COL, [(0, 6)])
    low = low + lax.ppermute(low, COL, [(0, 6), (2, 4)])
    high = high + lax.ppermute(high, COL, [(0, 2), (6, 4)])
    swap = [(0, 1), (2, 3), (4, 5), (6, 7)]
    low = low + lax.ppermute(low, COL, swap)
    high = high + lax.ppermute(high, COL, swap)
    return jnp.concatenate([low, high], axis=0)


def shards(matrix):
    rows = lax.axis_size("row")
    total_rows = matrix.shape[0] * rows
    col = lax.axis_index(COL)
    me = lax.axis_index("row")
    own_panel = matrix[:, :PANEL]

    gram = dot(own_panel, own_panel, ((0,), (0,)), EXACT)
    piece = lax.all_to_all(gram.reshape(rows, PANEL // rows, PANEL), "row", 0, 0, tiled=True).sum(0)
    piece = from_everyone(piece, COL)[0]
    gram = from_everyone(piece, "row").reshape(PANEL, PANEL)
    lower = jnp.linalg.cholesky(gram)
    inverse = jax.scipy.linalg.solve_triangular(lower, jnp.eye(PANEL, dtype=jnp.float32), lower=True)

    panel = spread_panel(own_panel, col)
    product = dot(matrix, panel, ((0,), (0,)), HIGH)
    width = product.shape[0] // rows
    share = lax.all_to_all(product.reshape(rows, width, PANEL), "row", 0, 0, tiled=True).sum(0)
    product = from_everyone(share, "row").reshape(rows * width, PANEL)

    block = PANEL // rows
    mine = lax.dynamic_slice(inverse, (me * block, 0), (block, PANEL))
    upper = dot(mine, product, ((1,), (1,)), EXACT)
    coefficients = dot(product, inverse, ((1,), (1,)), EXACT)
    weights = dot(coefficients, inverse, ((1,), (0,)), EXACT)
    scale = jnp.sqrt(jnp.float32(total_rows))
    holds = col == 0
    weights = jnp.concatenate(
        [jnp.where(holds, -scale * inverse, weights[:PANEL]), weights[PANEL:]], axis=0
    )
    is_panel = (lax.broadcasted_iota(jnp.int32, matrix.shape, 1) < PANEL) & holds
    reduced = jnp.where(is_panel, 0.0, matrix) - dot(panel, weights, ((1,), (1,)), HIGH)
    return (upper, reduced)


def solution(mesh):
    finer = Mesh(mesh.devices.reshape(mesh.shape["row"], 4, 2), ("row", *COL))
    return jax.shard_map(
        shards,
        mesh=finer,
        in_specs=(P("row", COL),),
        out_specs=(P("row", COL), P("row", COL)),
        check_vma=False,
    )
```

```python
import jax
import jax.numpy as jnp
from jax import lax
from jax.experimental import pallas as pl
from jax.experimental.pallas import tpu as pltpu
from jax.sharding import Mesh
from jax.sharding import PartitionSpec as P

PANEL = 256
COL = ("z", "c")
EXACT = lax.Precision.HIGHEST
F32 = jnp.float32
BLOCK, SUB, LANES = 32, 8, 128
ROWS = 512


def eliminate(strip, start):
    groups = BLOCK // SUB
    row_id = lax.broadcasted_iota(jnp.int32, (SUB, LANES), 0)
    lane_id = lax.broadcasted_iota(jnp.int32, (SUB, LANES), 1)
    half, lane0 = divmod(start, LANES)
    tiles = [list(t) for t in strip]
    diagonal = [jnp.zeros((SUB, LANES), F32) for _ in range(groups)]
    panel = 16
    for p in range(0, BLOCK, panel):
        g0 = p // SUB
        cols = {
            k: {g: jnp.broadcast_to(tiles[g][half][:, lane0 + k : lane0 + k + 1], (SUB, LANES)) for g in range(g0, groups)}
            for k in range(p, p + panel)
        }
        for j in range(p, p + panel):
            gj, sj = divmod(j, SUB)
            pivot = jnp.broadcast_to(cols[j][gj][sj : sj + 1], (SUB, LANES))
            diagonal[gj] = jnp.where(row_id == sj, pivot, diagonal[gj])
            inverse = 1.0 / pivot
            factor = {g: cols[j][g] * inverse for g in range(gj, groups)}
            factor[gj] = jnp.where(row_id > sj, factor[gj], 0.0)
            for k in range(j + 1, p + panel):
                row = jnp.broadcast_to(cols[k][gj][sj : sj + 1], (SUB, LANES))
                for g in range(gj, groups):
                    cols[k][g] = cols[k][g] - factor[g] * row
            for h in range(2):
                source = tiles[gj][h][sj : sj + 1]
                if h == half:
                    source = jnp.where(lane_id[0:1] == lane0 + j, 1.0, source)
                row = jnp.broadcast_to(source, (SUB, LANES))
                for g in range(gj, groups):
                    tile = tiles[g][h]
                    if h == half:
                        tile = jnp.where((lane_id == lane0 + j) & ((row_id > sj) if g == gj else True), 0.0, tile)
                    tiles[g][h] = tile - factor[g] * row
                if h == half:
                    tiles[gj][h] = jnp.where((lane_id == lane0 + j) & (row_id == sj), 1.0, tiles[gj][h])
    out = []
    for g in range(groups):
        r = lax.rsqrt(diagonal[g])
        r = r * (1.5 - 0.5 * diagonal[g] * r * r)
        above = (lane_id > lane0 + g * SUB + row_id) & (lane_id < lane0 + BLOCK)
        tiles[g][half] = jnp.where(above, 0.0, tiles[g][half])
        out.append([tiles[g][h] * r for h in range(2)])
    return out


def factor(work, inverse):
    n = work.shape[0]
    col_id = lax.broadcasted_iota(jnp.int32, (BLOCK, n), 1)
    for start in range(0, n, BLOCK):
        strip = [
            [work[start + SUB * g : start + SUB * (g + 1), LANES * h : LANES * (h + 1)] for h in range(2)]
            for g in range(BLOCK // SUB)
        ]
        done = eliminate(strip, start)
        rows = jnp.concatenate([jnp.concatenate(t, axis=1) for t in done], axis=0)
        inverse[start : start + BLOCK, :] = jnp.where(col_id < start + BLOCK, rows, 0.0)
        after = start + BLOCK
        for lo, hi in ((after, after + BLOCK), (after + BLOCK, n)):
            if lo >= n or lo >= hi:
                continue
            base = work[lo:hi, :]
            ids = lax.broadcasted_iota(jnp.int32, (hi - lo, n), 1)
            base = jnp.where((ids >= start) & (ids < after), 0.0, base)
            step = dot(rows[:, lo:hi], rows, ((0,), (0,)), EXACT)
            work[lo:hi, :] = base - step


def dot(left, right, contract, precision=None):
    return lax.dot_general(
        left, right, (contract, ((), ())), precision=precision, preferred_element_type=F32
    )


def split(value):
    high = value.astype(jnp.bfloat16)
    return high, (value - high.astype(F32)).astype(jnp.bfloat16)


NN = ((1,), (0,))


def split_dot(left, right):
    return dot(left[0], right[0], NN) + (dot(left[0], right[1], NN) + dot(left[1], right[0], NN))


def prepare_kernel(matrix, high, low):
    high[...], low[...] = split(matrix[...])


def product_kernel(low, low_more, high, high_more, matrix_high, matrix_low, out, panel_high, panel_low):
    half = low.shape[0]
    cols = matrix_high.shape[1]
    for first, more, start in ((low, low_more, 0), (high, high_more, half)):
        part = slice(start, start + half)
        panel = first[...] + more[...]
        panel_high[part], panel_low[part] = split(panel)
        turned = panel.T
        pieces = split(turned)
        for c in range(0, cols, PANEL):
            here = slice(c, c + PANEL)
            value = split_dot(pieces, (matrix_high[part, here], matrix_low[part, here]))
            out[:, here] = value if start == 0 else out[:, here] + value
        value = dot(turned, panel, NN, EXACT)
        out[:, cols:] = value if start == 0 else out[:, cols:] + value


def finish_kernel(place, gathered, panel_high, panel_low, matrix, upper, out, work, inverse, coeff, coeff_low, held, arrived, left):
    blocks = matrix.shape[0] // ROWS
    cols = matrix.shape[1]
    scale = float(matrix.shape[0] * (PANEL // upper.shape[0])) ** 0.5

    def fetch(b):
        part = slice(b * ROWS, b * ROWS + ROWS)
        return pltpu.make_async_copy(matrix.at[part], held.at[part], arrived.at[b])

    def send(b):
        part = slice(b * ROWS, b * ROWS + ROWS)
        return pltpu.make_async_copy(held.at[part], out.at[part], left.at[b])

    for b in range(blocks):
        fetch(b).start()
    holds = place[0] == 1
    work[...] = gathered[:, cols:]
    factor(work, inverse)
    lower = split(inverse[...])
    turned = inverse[...].T
    upward = split(turned)
    height = upper.shape[0]
    mine = pl.ds(pl.multiple_of(place[1] * height, height), height)
    for c in range(0, cols, PANEL):
        here = slice(c, c + PANEL)
        work[...] = split_dot(lower, split(gathered[:, here]))
        upper[:, here] = work[mine, :]
        weights = split_dot(upward, split(work[...]))
        if c == 0:
            weights = jnp.where(holds, -scale * turned, weights)
        coeff[:, here], coeff_low[:, here] = split(weights)

    for b in range(blocks):
        part = slice(b * ROWS, b * ROWS + ROWS)
        fetch(b).wait()
        panel = (panel_high[part], panel_low[part])
        for c in range(0, cols, PANEL):
            here = slice(c, c + PANEL)
            change = split_dot(panel, (coeff[:, here], coeff_low[:, here]))
            value = held[part, here]
            if c == 0:
                value = jnp.where(holds, 0.0, value)
            held[part, here] = value - change
        send(b).start()
    for b in range(blocks):
        send(b).wait()


VMEM = pl.BlockSpec(memory_space=pltpu.VMEM)
SMEM = pl.BlockSpec(memory_space=pltpu.SMEM)
HBM = pl.BlockSpec(memory_space=pltpu.HBM)


def prepare(matrix):
    shape = jax.ShapeDtypeStruct(matrix.shape, jnp.bfloat16)
    block = pl.BlockSpec((ROWS // 2, matrix.shape[1]), lambda i: (i, 0))
    return pl.pallas_call(
        prepare_kernel,
        grid=(2 * matrix.shape[0] // ROWS,),
        out_shape=(shape, shape),
        in_specs=[block],
        out_specs=(block, block),
        cost_estimate=pl.CostEstimate(flops=3 * 10**9, bytes_accessed=16 << 20, transcendentals=0),
    )(matrix)


def products(low, low_more, high, high_more, pieces):
    rows, cols = pieces[0].shape
    narrow = jax.ShapeDtypeStruct((rows, PANEL), jnp.bfloat16)
    return pl.pallas_call(
        product_kernel,
        out_shape=(jax.ShapeDtypeStruct((PANEL, cols + PANEL), F32), narrow, narrow),
        in_specs=[VMEM] * 6,
        out_specs=[VMEM] * 3,
        compiler_params=pltpu.CompilerParams(vmem_limit_bytes=32 << 20),
        cost_estimate=pl.CostEstimate(flops=5 * 10**9, bytes_accessed=16 << 20, transcendentals=0),
    )(low, low_more, high, high_more, *pieces)


def finish(place, gathered, panel_high, panel_low, matrix, height):
    rows, cols = matrix.shape
    return pl.pallas_call(
        finish_kernel,
        out_shape=(
            jax.ShapeDtypeStruct((height, cols), F32),
            jax.ShapeDtypeStruct(matrix.shape, F32),
        ),
        in_specs=[SMEM] + [VMEM] * 3 + [HBM],
        out_specs=[VMEM, HBM],
        scratch_shapes=[
            pltpu.VMEM((PANEL, PANEL), F32),
            pltpu.VMEM((PANEL, PANEL), F32),
            pltpu.VMEM((PANEL, cols), jnp.bfloat16),
            pltpu.VMEM((PANEL, cols), jnp.bfloat16),
            pltpu.VMEM(matrix.shape, F32),
            pltpu.SemaphoreType.DMA((rows // ROWS,)),
            pltpu.SemaphoreType.DMA((rows // ROWS,)),
        ],
        compiler_params=pltpu.CompilerParams(vmem_limit_bytes=50 << 20),
        cost_estimate=pl.CostEstimate(flops=8 * 10**9, bytes_accessed=24 << 20, transcendentals=0),
    )(place, gathered, panel_high, panel_low, matrix)


def from_everyone(shard, axis):
    copies = jnp.broadcast_to(shard, (lax.axis_size(axis), *shard.shape))
    return lax.all_to_all(copies, axis, 0, 0, tiled=True)


def sum_at_owner(shard, axis):
    count = lax.axis_size(axis)
    tiles = shard.reshape(count, shard.shape[0] // count, shard.shape[1])
    return lax.all_to_all(tiles, axis, 0, 0, tiled=True).sum(0)


def shards(matrix):
    holds = lax.axis_index(COL) == 0
    half = matrix.shape[0] // 2
    own_low, own_high = lax.optimization_barrier((matrix[:half, :PANEL], matrix[half:, :PANEL]))
    swap = [(0, 1), (2, 3), (4, 5), (6, 7)]
    low = lax.ppermute(own_low, COL, [(0, 2)])
    high = lax.ppermute(own_high, COL, [(0, 6)])
    low_too = lax.ppermute(own_low, COL, [(0, 6)])
    high_too = lax.ppermute(own_high, COL, [(0, 2)])
    pieces = prepare(matrix)
    low_relay = lax.ppermute(low, COL, [(2, 4)])
    high_relay = lax.ppermute(high, COL, [(6, 4)])
    low = jnp.where(holds, own_low, low + low_too + low_relay)
    high = jnp.where(holds, own_high, high + high_too + high_relay)
    low_more = lax.ppermute(low, COL, swap)
    high_more = lax.ppermute(high, COL, swap)
    product, panel_high, panel_low = products(low, low_more, high, high_more, pieces)
    share = sum_at_owner(product, "row")
    gathered = from_everyone(share, "row").reshape(product.shape)
    place = jnp.stack([holds.astype(jnp.int32), lax.axis_index("row").astype(jnp.int32)])
    upper, reduced = finish(place, gathered, panel_high, panel_low, matrix, share.shape[0])
    return (upper, reduced)


def solution(mesh):
    finer = Mesh(mesh.devices.reshape(mesh.shape["row"], 4, 2), ("row", *COL))
    return jax.shard_map(
        shards,
        mesh=finer,
        in_specs=(P("row", COL),),
        out_specs=(P("row", COL), P("row", COL)),
        check_vma=False,
    )
```

```python
import jax
import jax.numpy as jnp
from jax import lax
from jax.experimental import pallas as pl
from jax.experimental.pallas import tpu as pltpu
from jax.sharding import Mesh
from jax.sharding import PartitionSpec as P

PANEL = 256
COL = ("z", "c")
EXACT = lax.Precision.HIGHEST
F32 = jnp.float32
BLOCK, SUB, LANES = 32, 8, 128
ROWS = 512


def eliminate(strip, start):
    groups = BLOCK // SUB
    row_id = lax.broadcasted_iota(jnp.int32, (SUB, LANES), 0)
    lane_id = lax.broadcasted_iota(jnp.int32, (SUB, LANES), 1)
    half, lane0 = divmod(start, LANES)
    tiles = [list(t) for t in strip]
    diagonal = [jnp.zeros((SUB, LANES), F32) for _ in range(groups)]
    panel = 16
    for p in range(0, BLOCK, panel):
        g0 = p // SUB
        cols = {
            k: {g: jnp.broadcast_to(tiles[g][half][:, lane0 + k : lane0 + k + 1], (SUB, LANES)) for g in range(g0, groups)}
            for k in range(p, p + panel)
        }
        for j in range(p, p + panel):
            gj, sj = divmod(j, SUB)
            pivot = jnp.broadcast_to(cols[j][gj][sj : sj + 1], (SUB, LANES))
            diagonal[gj] = jnp.where(row_id == sj, pivot, diagonal[gj])
            inverse = 1.0 / pivot
            below = {g: cols[j][g] for g in range(gj, groups)}
            below[gj] = jnp.where(row_id > sj, below[gj], 0.0)
            factor = {g: below[g] * inverse for g in range(gj, groups)}
            for k in range(j + 1, p + panel):
                row = jnp.broadcast_to(cols[k][gj][sj : sj + 1], (SUB, LANES))
                for g in range(gj, groups):
                    if k == j + 1:
                        cols[k][g] = cols[k][g] - (below[g] * row) * inverse
                    else:
                        cols[k][g] = cols[k][g] - factor[g] * row
            for h in range(2):
                source = tiles[gj][h][sj : sj + 1]
                if h == half:
                    source = jnp.where(lane_id[0:1] == lane0 + j, 1.0, source)
                row = jnp.broadcast_to(source, (SUB, LANES))
                for g in range(gj, groups):
                    tile = tiles[g][h]
                    if h == half:
                        tile = jnp.where((lane_id == lane0 + j) & ((row_id > sj) if g == gj else True), 0.0, tile)
                    tiles[g][h] = tile - factor[g] * row
                if h == half:
                    tiles[gj][h] = jnp.where((lane_id == lane0 + j) & (row_id == sj), 1.0, tiles[gj][h])
    out = []
    for g in range(groups):
        r = lax.rsqrt(diagonal[g])
        r = r * (1.5 - 0.5 * diagonal[g] * r * r)
        above = (lane_id > lane0 + g * SUB + row_id) & (lane_id < lane0 + BLOCK)
        tiles[g][half] = jnp.where(above, 0.0, tiles[g][half])
        out.append([tiles[g][h] * r for h in range(2)])
    return out


def factor(work, inverse):
    n = work.shape[0]
    col_id = lax.broadcasted_iota(jnp.int32, (BLOCK, n), 1)
    for start in range(0, n, BLOCK):
        strip = [
            [work[start + SUB * g : start + SUB * (g + 1), LANES * h : LANES * (h + 1)] for h in range(2)]
            for g in range(BLOCK // SUB)
        ]
        done = eliminate(strip, start)
        rows = jnp.concatenate([jnp.concatenate(t, axis=1) for t in done], axis=0)
        inverse[start : start + BLOCK, :] = jnp.where(col_id < start + BLOCK, rows, 0.0)
        after = start + BLOCK
        for lo, hi in ((after, after + BLOCK), (after + BLOCK, n)):
            if lo >= n or lo >= hi:
                continue
            base = work[lo:hi, :]
            ids = lax.broadcasted_iota(jnp.int32, (hi - lo, n), 1)
            base = jnp.where((ids >= start) & (ids < after), 0.0, base)
            step = dot(rows[:, lo:hi], rows, ((0,), (0,)), EXACT)
            work[lo:hi, :] = base - step


def dot(left, right, contract, precision=None):
    return lax.dot_general(
        left, right, (contract, ((), ())), precision=precision, preferred_element_type=F32
    )


def split(value):
    high = value.astype(jnp.bfloat16)
    return high, (value - high.astype(F32)).astype(jnp.bfloat16)


NN = ((1,), (0,))


def split_dot(left, right):
    return dot(left[0], right[0], NN) + (dot(left[0], right[1], NN) + dot(left[1], right[0], NN))


def prepare_kernel(matrix, high, low):
    high[...], low[...] = split(matrix[...])


def pick_kernel(place, *refs):
    sources, out, done = refs[:-2], refs[-2], refs[-1]
    for z in range(4):

        @pl.when(place[2] == z)
        def _():
            copies = []
            begin = 0
            for source in sources[2 * z : 2 * z + 2]:
                step = source.shape[0] // 4
                for i in range(4):
                    copies.append(
                        pltpu.make_async_copy(
                            source.at[i * step : (i + 1) * step],
                            out.at[begin + i * step : begin + (i + 1) * step],
                            done.at[len(copies)],
                        )
                    )
                begin += source.shape[0]
            for copy in copies:
                copy.start()
            for copy in copies:
                copy.wait()


def product_kernel(place, panel_here, panel_sent, upper_pieces, upper_rest, lower_pieces, lower_rest, out, panel_high, panel_low):
    half, cols = upper_pieces.shape
    sent = place[3] == 1
    for start, matrix_high, matrix_low in ((0, upper_pieces, upper_rest), (half, lower_pieces, lower_rest)):
        part = slice(start, start + half)
        panel = jnp.where(sent, panel_sent[part], panel_here[part])
        first, second = split(panel)
        third = ((panel - first.astype(F32)) - second.astype(F32)).astype(jnp.bfloat16)
        panel_high[part] = first
        panel_low[part] = second
        pieces = split(panel.T)
        for c in range(0, cols, PANEL):
            here = slice(c, c + PANEL)
            value = split_dot(pieces, (matrix_high[:, here], matrix_low[:, here]))
            out[:, here] = value if start == 0 else out[:, here] + value
        cross = dot(pieces[0], second, NN) + dot(pieces[0], third, NN)
        value = dot(pieces[0], first, NN) + (dot(pieces[1], second, NN) + (cross + cross.T))
        out[:, cols:] = value if start == 0 else out[:, cols:] + value


def finish_kernel(place, gathered, panel_high, panel_low, matrix, upper, out, work, inverse, found, coeff, coeff_low, held, arrived, left):
    blocks = matrix.shape[0] // ROWS
    cols = matrix.shape[1]
    scale = float(matrix.shape[0] * (PANEL // upper.shape[0])) ** 0.5

    def fetch(b):
        part = slice(b * ROWS, b * ROWS + ROWS)
        return pltpu.make_async_copy(matrix.at[part], held.at[part], arrived.at[b])

    def send(b):
        part = slice(b * ROWS, b * ROWS + ROWS)
        return pltpu.make_async_copy(held.at[part], out.at[part], left.at[b])

    for b in range(blocks):
        fetch(b).start()
    holds = place[0] == 1
    work[...] = gathered[:, cols:]
    factor(work, inverse)
    lower = split(inverse[...])
    turned = inverse[...].T
    upward = split(turned)
    height = upper.shape[0]
    mine = pl.ds(pl.multiple_of(place[1] * height, height), height)
    for c in range(0, cols, PANEL):
        here = slice(c, c + PANEL)
        part = split_dot(lower, split(gathered[:, here]))
        found[:, here] = part
        weights = split_dot(upward, split(part))
        if c == 0:
            weights = jnp.where(holds, -scale * turned, weights)
        coeff[:, here], coeff_low[:, here] = split(weights)
    upper[...] = found[mine, :]

    for b in range(blocks):
        part = slice(b * ROWS, b * ROWS + ROWS)
        fetch(b).wait()
        panel = (panel_high[part], panel_low[part])
        for c in range(0, cols, PANEL):
            here = slice(c, c + PANEL)
            change = split_dot(panel, (coeff[:, here], coeff_low[:, here]))
            value = held[part, here]
            if c == 0:
                value = jnp.where(holds, 0.0, value)
            held[part, here] = value - change
        send(b).start()
    for b in range(blocks):
        send(b).wait()


VMEM = pl.BlockSpec(memory_space=pltpu.VMEM)
SMEM = pl.BlockSpec(memory_space=pltpu.SMEM)
HBM = pl.BlockSpec(memory_space=pltpu.HBM)


def prepare(matrix, part=0, parts=1):
    count = 2 * matrix.shape[0] // ROWS // parts
    shape = jax.ShapeDtypeStruct((matrix.shape[0] // parts, matrix.shape[1]), jnp.bfloat16)
    block = pl.BlockSpec((ROWS // 2, matrix.shape[1]), lambda i: (i, 0))
    return pl.pallas_call(
        prepare_kernel,
        grid=(count,),
        out_shape=(shape, shape),
        in_specs=[pl.BlockSpec((ROWS // 2, matrix.shape[1]), lambda i: (i + part * count, 0))],
        out_specs=(block, block),
        compiler_params=pltpu.CompilerParams(vmem_limit_bytes=12 << 20),
        cost_estimate=pl.CostEstimate(flops=2 * 10**9, bytes_accessed=8 << 20, transcendentals=0),
    )(matrix)


def pick(place, sources):
    low, width = sources[0].shape
    high = sources[1].shape[0]
    return pl.pallas_call(
        pick_kernel,
        out_shape=jax.ShapeDtypeStruct((low + high, width), F32),
        in_specs=[SMEM] + [HBM] * len(sources),
        out_specs=VMEM,
        scratch_shapes=[pltpu.SemaphoreType.DMA((8,))],
        compiler_params=pltpu.CompilerParams(vmem_limit_bytes=8 << 20),
        cost_estimate=pl.CostEstimate(flops=10**8, bytes_accessed=4 << 20, transcendentals=0),
    )(place, *sources)


def products(place, panel_here, panel_sent, pieces):
    rows, cols = panel_here.shape[0], pieces[0].shape[1]
    narrow = jax.ShapeDtypeStruct((rows, PANEL), jnp.bfloat16)
    return pl.pallas_call(
        product_kernel,
        out_shape=(jax.ShapeDtypeStruct((PANEL, cols + PANEL), F32), narrow, narrow),
        in_specs=[SMEM] + [VMEM] * 6,
        out_specs=[VMEM] * 3,
        compiler_params=pltpu.CompilerParams(vmem_limit_bytes=32 << 20),
        cost_estimate=pl.CostEstimate(flops=5 * 10**9, bytes_accessed=16 << 20, transcendentals=0),
    )(place, panel_here, panel_sent, *pieces)


def finish(place, gathered, panel_high, panel_low, matrix, height):
    rows, cols = matrix.shape
    return pl.pallas_call(
        finish_kernel,
        out_shape=(
            jax.ShapeDtypeStruct((height, cols), F32),
            jax.ShapeDtypeStruct(matrix.shape, F32),
        ),
        in_specs=[SMEM] + [VMEM] * 3 + [HBM],
        out_specs=[VMEM, HBM],
        scratch_shapes=[
            pltpu.VMEM((PANEL, PANEL), F32),
            pltpu.VMEM((PANEL, PANEL), F32),
            pltpu.VMEM((PANEL, cols), F32),
            pltpu.VMEM((PANEL, cols), jnp.bfloat16),
            pltpu.VMEM((PANEL, cols), jnp.bfloat16),
            pltpu.VMEM(matrix.shape, F32),
            pltpu.SemaphoreType.DMA((rows // ROWS,)),
            pltpu.SemaphoreType.DMA((rows // ROWS,)),
        ],
        compiler_params=pltpu.CompilerParams(vmem_limit_bytes=50 << 20),
        cost_estimate=pl.CostEstimate(flops=8 * 10**9, bytes_accessed=24 << 20, transcendentals=0),
    )(place, gathered, panel_high, panel_low, matrix)


def from_everyone(shard, axis):
    copies = jnp.broadcast_to(shard, (lax.axis_size(axis), *shard.shape))
    return lax.all_to_all(copies, axis, 0, 0, tiled=True)


def sum_at_owner(shard, axis):
    count = lax.axis_size(axis)
    tiles = shard.reshape(count, shard.shape[0] // count, shard.shape[1])
    return lax.all_to_all(tiles, axis, 0, 0, tiled=True).sum(0)


def shards(matrix):
    col = lax.axis_index(COL)
    place = jnp.stack([col == 0, lax.axis_index("row"), col // 2, col % 2]).astype(jnp.int32)
    half = matrix.shape[0] * 35 // 64
    own_low = lax.optimization_barrier(matrix[:half, :PANEL])
    own_high = lax.optimization_barrier(matrix[half:, :PANEL])
    first_low = lax.ppermute(own_low, COL, [(0, 2)])
    first_high = lax.ppermute(own_high, COL, [(0, 6)])
    second_low = lax.ppermute(own_low, COL, [(0, 6)])
    second_high = lax.ppermute(own_high, COL, [(0, 2)])
    pieces = prepare(matrix, 0, 2)
    pieces += prepare(matrix, 1, 2)
    relay_low = lax.ppermute(first_low, COL, [(2, 4)])
    relay_high = lax.ppermute(first_high, COL, [(6, 4)])
    here = pick(place, (own_low, own_high, first_low, second_high, relay_low, relay_high, second_low, first_high))
    sent = lax.ppermute(here, COL, [(0, 1), (2, 3), (4, 5), (6, 7)])
    product, panel_high, panel_low = products(place, here, sent, pieces)
    share = sum_at_owner(product, "row")
    gathered = from_everyone(share, "row").reshape(product.shape)
    upper, reduced = finish(place, gathered, panel_high, panel_low, matrix, share.shape[0])
    return (upper, reduced)


def solution(mesh):
    finer = Mesh(mesh.devices.reshape(mesh.shape["row"], 4, 2), ("row", *COL))
    return jax.shard_map(
        shards,
        mesh=finer,
        in_specs=(P("row", COL),),
        out_specs=(P("row", COL), P("row", COL)),
        check_vma=False,
    )
```

```python
import jax
import jax.numpy as jnp
from jax import lax
from jax.experimental import pallas as pl
from jax.experimental.pallas import tpu as pltpu
from jax.sharding import Mesh
from jax.sharding import PartitionSpec as P

PANEL = 256
COL = ("z", "c")
EXACT = lax.Precision.HIGHEST
F32 = jnp.float32
BLOCK, SUB, LANES = 32, 8, 128
ROWS = 512


def eliminate(strip, start):
    groups = BLOCK // SUB
    row_id = lax.broadcasted_iota(jnp.int32, (SUB, LANES), 0)
    lane_id = lax.broadcasted_iota(jnp.int32, (SUB, LANES), 1)
    half, lane0 = divmod(start, LANES)
    tiles = [list(t) for t in strip]
    diagonal = [jnp.zeros((SUB, LANES), F32) for _ in range(groups)]
    panel = 16
    for p in range(0, BLOCK, panel):
        g0 = p // SUB
        cols = {
            k: {g: jnp.broadcast_to(tiles[g][half][:, lane0 + k : lane0 + k + 1], (SUB, LANES)) for g in range(g0, groups)}
            for k in range(p, p + panel)
        }
        for j in range(p, p + panel):
            gj, sj = divmod(j, SUB)
            pivot = jnp.broadcast_to(cols[j][gj][sj : sj + 1], (SUB, LANES))
            diagonal[gj] = jnp.where(row_id == sj, pivot, diagonal[gj])
            inverse = 1.0 / pivot
            below = {g: cols[j][g] for g in range(gj, groups)}
            below[gj] = jnp.where(row_id > sj, below[gj], 0.0)
            factor = {g: below[g] * inverse for g in range(gj, groups)}
            for k in range(j + 1, p + panel):
                row = jnp.broadcast_to(cols[k][gj][sj : sj + 1], (SUB, LANES))
                for g in range(gj, groups):
                    if k == j + 1:
                        cols[k][g] = cols[k][g] - (below[g] * row) * inverse
                    else:
                        cols[k][g] = cols[k][g] - factor[g] * row
            for h in range(2):
                source = tiles[gj][h][sj : sj + 1]
                if h == half:
                    source = jnp.where(lane_id[0:1] == lane0 + j, 1.0, source)
                row = jnp.broadcast_to(source, (SUB, LANES))
                for g in range(gj, groups):
                    tile = tiles[g][h]
                    if h == half:
                        tile = jnp.where((lane_id == lane0 + j) & ((row_id > sj) if g == gj else True), 0.0, tile)
                    tiles[g][h] = tile - factor[g] * row
                if h == half:
                    tiles[gj][h] = jnp.where((lane_id == lane0 + j) & (row_id == sj), 1.0, tiles[gj][h])
    out = []
    for g in range(groups):
        r = lax.rsqrt(diagonal[g])
        r = r * (1.5 - 0.5 * diagonal[g] * r * r)
        above = (lane_id > lane0 + g * SUB + row_id) & (lane_id < lane0 + BLOCK)
        tiles[g][half] = jnp.where(above, 0.0, tiles[g][half])
        out.append([tiles[g][h] * r for h in range(2)])
    return out


def factor(work, inverse):
    n = work.shape[0]
    col_id = lax.broadcasted_iota(jnp.int32, (BLOCK, n), 1)
    for start in range(0, n, BLOCK):
        strip = [
            [work[start + SUB * g : start + SUB * (g + 1), LANES * h : LANES * (h + 1)] for h in range(2)]
            for g in range(BLOCK // SUB)
        ]
        done = eliminate(strip, start)
        rows = jnp.concatenate([jnp.concatenate(t, axis=1) for t in done], axis=0)
        inverse[start : start + BLOCK, :] = jnp.where(col_id < start + BLOCK, rows, 0.0)
        after = start + BLOCK
        for lo, hi in ((after, after + BLOCK), (after + BLOCK, n)):
            if lo >= n or lo >= hi:
                continue
            base = work[lo:hi, :]
            ids = lax.broadcasted_iota(jnp.int32, (hi - lo, n), 1)
            base = jnp.where((ids >= start) & (ids < after), 0.0, base)
            step = dot(rows[:, lo:hi], rows, ((0,), (0,)), EXACT)
            work[lo:hi, :] = base - step


def dot(left, right, contract, precision=None):
    return lax.dot_general(
        left, right, (contract, ((), ())), precision=precision, preferred_element_type=F32
    )


def split(value):
    high = value.astype(jnp.bfloat16)
    return high, (value - high.astype(F32)).astype(jnp.bfloat16)


NN = ((1,), (0,))


def split_dot(left, right):
    return dot(left[0], right[0], NN) + (dot(left[0], right[1], NN) + dot(left[1], right[0], NN))


def prepare_kernel(matrix, high, low):
    high[...], low[...] = split(matrix[...])


def pick_kernel(place, *refs):
    sources, out, done = refs[:-2], refs[-2], refs[-1]
    for z in range(4):

        @pl.when(place[2] == z)
        def _():
            copies = []
            begin = 0
            for source in sources[2 * z : 2 * z + 2]:
                step = source.shape[0] // 4
                for i in range(4):
                    copies.append(
                        pltpu.make_async_copy(
                            source.at[i * step : (i + 1) * step],
                            out.at[begin + i * step : begin + (i + 1) * step],
                            done.at[len(copies)],
                        )
                    )
                begin += source.shape[0]
            for copy in copies:
                copy.start()
            for copy in copies:
                copy.wait()


def product_kernel(place, panel_here, panel_sent, upper_pieces, upper_rest, lower_pieces, lower_rest, out, panel_high, panel_low):
    half, cols = upper_pieces.shape
    sent = place[3] == 1
    for start, matrix_high, matrix_low in ((0, upper_pieces, upper_rest), (half, lower_pieces, lower_rest)):
        part = slice(start, start + half)
        panel = jnp.where(sent, panel_sent[part], panel_here[part])
        first, second = split(panel)
        third = ((panel - first.astype(F32)) - second.astype(F32)).astype(jnp.bfloat16)
        panel_high[part] = first
        panel_low[part] = second
        pieces = split(panel.T)
        for c in range(0, cols, PANEL):
            here = slice(c, c + PANEL)
            value = split_dot(pieces, (matrix_high[:, here], matrix_low[:, here]))
            out[:, here] = value if start == 0 else out[:, here] + value
        cross = dot(pieces[0], second, NN) + dot(pieces[0], third, NN)
        value = dot(pieces[0], first, NN) + (dot(pieces[1], second, NN) + (cross + cross.T))
        out[:, cols:] = value if start == 0 else out[:, cols:] + value


def finish_kernel(place, gathered, panel_high, panel_low, matrix, upper, out, work, inverse, found, coeff, coeff_low, held, arrived, left):
    blocks = matrix.shape[0] // ROWS
    cols = matrix.shape[1]
    scale = float(matrix.shape[0] * (PANEL // upper.shape[0])) ** 0.5

    def fetch(b):
        part = slice(b * ROWS, b * ROWS + ROWS)
        return pltpu.make_async_copy(matrix.at[part], held.at[part], arrived.at[b])

    def send(b):
        part = slice(b * ROWS, b * ROWS + ROWS)
        return pltpu.make_async_copy(held.at[part], out.at[part], left.at[b])

    for b in range(blocks):
        fetch(b).start()
    holds = place[0] == 1
    work[...] = gathered[:, cols:]
    factor(work, inverse)
    lower = split(inverse[...])
    turned = inverse[...].T
    upward = split(turned)
    height = upper.shape[0]
    mine = pl.ds(pl.multiple_of(place[1] * height, height), height)
    for c in range(0, cols, PANEL):
        here = slice(c, c + PANEL)
        part = split_dot(lower, split(gathered[:, here]))
        found[:, here] = part
        weights = split_dot(upward, split(part))
        if c == 0:
            weights = jnp.where(holds, -scale * turned, weights)
        coeff[:, here], coeff_low[:, here] = split(weights)
    upper[...] = found[mine, :]

    for b in range(blocks):
        part = slice(b * ROWS, b * ROWS + ROWS)
        fetch(b).wait()
        panel = (panel_high[part], panel_low[part])
        for c in range(0, cols, PANEL):
            here = slice(c, c + PANEL)
            change = split_dot(panel, (coeff[:, here], coeff_low[:, here]))
            value = held[part, here]
            if c == 0:
                value = jnp.where(holds, 0.0, value)
            held[part, here] = value - change
        send(b).start()
    for b in range(blocks):
        send(b).wait()


VMEM = pl.BlockSpec(memory_space=pltpu.VMEM)
SMEM = pl.BlockSpec(memory_space=pltpu.SMEM)
HBM = pl.BlockSpec(memory_space=pltpu.HBM)


def prepare(matrix, part=0, parts=1):
    count = 2 * matrix.shape[0] // ROWS // parts
    shape = jax.ShapeDtypeStruct((matrix.shape[0] // parts, matrix.shape[1]), jnp.bfloat16)
    block = pl.BlockSpec((ROWS // 2, matrix.shape[1]), lambda i: (i, 0))
    return pl.pallas_call(
        prepare_kernel,
        grid=(count,),
        out_shape=(shape, shape),
        in_specs=[pl.BlockSpec((ROWS // 2, matrix.shape[1]), lambda i: (i + part * count, 0))],
        out_specs=(block, block),
        compiler_params=pltpu.CompilerParams(vmem_limit_bytes=12 << 20),
        cost_estimate=pl.CostEstimate(flops=2 * 10**9, bytes_accessed=8 << 20, transcendentals=0),
    )(matrix)


def pick(place, sources):
    low, width = sources[0].shape
    high = sources[1].shape[0]
    return pl.pallas_call(
        pick_kernel,
        out_shape=jax.ShapeDtypeStruct((low + high, width), F32),
        in_specs=[SMEM] + [HBM] * len(sources),
        out_specs=VMEM,
        scratch_shapes=[pltpu.SemaphoreType.DMA((8,))],
        compiler_params=pltpu.CompilerParams(vmem_limit_bytes=8 << 20),
        cost_estimate=pl.CostEstimate(flops=10**8, bytes_accessed=4 << 20, transcendentals=0),
    )(place, *sources)


def products(place, panel_here, panel_sent, pieces):
    rows, cols = panel_here.shape[0], pieces[0].shape[1]
    narrow = jax.ShapeDtypeStruct((rows, PANEL), jnp.bfloat16)
    return pl.pallas_call(
        product_kernel,
        out_shape=(jax.ShapeDtypeStruct((PANEL, cols + PANEL), F32), narrow, narrow),
        in_specs=[SMEM] + [VMEM] * 6,
        out_specs=[VMEM] * 3,
        compiler_params=pltpu.CompilerParams(vmem_limit_bytes=32 << 20),
        cost_estimate=pl.CostEstimate(flops=5 * 10**9, bytes_accessed=16 << 20, transcendentals=0),
    )(place, panel_here, panel_sent, *pieces)


def finish(place, gathered, panel_high, panel_low, matrix, height):
    rows, cols = matrix.shape
    return pl.pallas_call(
        finish_kernel,
        out_shape=(
            jax.ShapeDtypeStruct((height, cols), F32),
            jax.ShapeDtypeStruct(matrix.shape, F32),
        ),
        in_specs=[SMEM] + [VMEM] * 3 + [HBM],
        out_specs=[VMEM, HBM],
        scratch_shapes=[
            pltpu.VMEM((PANEL, PANEL), F32),
            pltpu.VMEM((PANEL, PANEL), F32),
            pltpu.VMEM((PANEL, cols), F32),
            pltpu.VMEM((PANEL, cols), jnp.bfloat16),
            pltpu.VMEM((PANEL, cols), jnp.bfloat16),
            pltpu.VMEM(matrix.shape, F32),
            pltpu.SemaphoreType.DMA((rows // ROWS,)),
            pltpu.SemaphoreType.DMA((rows // ROWS,)),
        ],
        compiler_params=pltpu.CompilerParams(vmem_limit_bytes=50 << 20),
        cost_estimate=pl.CostEstimate(flops=8 * 10**9, bytes_accessed=24 << 20, transcendentals=0),
    )(place, gathered, panel_high, panel_low, matrix)


def total_kernel(tiles, out):
    total = tiles[0]
    for i in range(1, tiles.shape[0]):
        total = total + tiles[i]
    for i in range(out.shape[0]):
        out[i] = total


def exchange(tiles):
    return lax.all_to_all(tiles, "row", 0, 0, tiled=True)


def sum_everywhere(value):
    count = lax.axis_size("row")
    tiles = exchange(value.reshape(count, value.shape[0] // count, value.shape[1]))
    copies = pl.pallas_call(
        total_kernel,
        out_shape=jax.ShapeDtypeStruct(tiles.shape, F32),
        in_specs=[VMEM],
        out_specs=VMEM,
        compiler_params=pltpu.CompilerParams(vmem_limit_bytes=8 << 20),
        cost_estimate=pl.CostEstimate(flops=10**7, bytes_accessed=3 << 20, transcendentals=0),
    )(tiles)
    return exchange(copies).reshape(value.shape)


def shards(matrix):
    col = lax.axis_index(COL)
    place = jnp.stack([col == 0, lax.axis_index("row"), col // 2, col % 2]).astype(jnp.int32)
    half = matrix.shape[0] * 35 // 64
    own_low = lax.optimization_barrier(matrix[:half, :PANEL])
    own_high = lax.optimization_barrier(matrix[half:, :PANEL])
    first_low = lax.ppermute(own_low, COL, [(0, 2)])
    first_high = lax.ppermute(own_high, COL, [(0, 6)])
    second_low = lax.ppermute(own_low, COL, [(0, 6)])
    second_high = lax.ppermute(own_high, COL, [(0, 2)])
    pieces = prepare(matrix, 0, 2)
    pieces += prepare(matrix, 1, 2)
    relay_low = lax.ppermute(first_low, COL, [(2, 4)])
    relay_high = lax.ppermute(first_high, COL, [(6, 4)])
    here = pick(place, (own_low, own_high, first_low, second_high, relay_low, relay_high, second_low, first_high))
    sent = lax.ppermute(here, COL, [(0, 1), (2, 3), (4, 5), (6, 7)])
    product, panel_high, panel_low = products(place, here, sent, pieces)
    gathered = sum_everywhere(product)
    height = PANEL // lax.axis_size("row")
    upper, reduced = finish(place, gathered, panel_high, panel_low, matrix, height)
    return (upper, reduced)


def solution(mesh):
    finer = Mesh(mesh.devices.reshape(mesh.shape["row"], 4, 2), ("row", *COL))
    return jax.shard_map(
        shards,
        mesh=finer,
        in_specs=(P("row", COL),),
        out_specs=(P("row", COL), P("row", COL)),
        check_vma=False,
    )
```

```python
import jax
import jax.numpy as jnp
from jax import lax
from jax.experimental import pallas as pl
from jax.experimental.pallas import tpu as pltpu
from jax.sharding import Mesh
from jax.sharding import PartitionSpec as P

PANEL = 256
COL = ("z", "c")
EXACT = lax.Precision.HIGHEST
F32 = jnp.float32
BLOCK, SUB, LANES = 32, 8, 128
ROWS = 512


def eliminate(strip, start):
    groups = BLOCK // SUB
    row_id = lax.broadcasted_iota(jnp.int32, (SUB, LANES), 0)
    lane_id = lax.broadcasted_iota(jnp.int32, (SUB, LANES), 1)
    half, lane0 = divmod(start, LANES)
    tiles = [list(t) for t in strip]
    diagonal = [jnp.zeros((SUB, LANES), F32) for _ in range(groups)]
    panel = 16
    for p in range(0, BLOCK, panel):
        g0 = p // SUB
        cols = {
            k: {g: jnp.broadcast_to(tiles[g][half][:, lane0 + k : lane0 + k + 1], (SUB, LANES)) for g in range(g0, groups)}
            for k in range(p, p + panel)
        }
        for j in range(p, p + panel):
            gj, sj = divmod(j, SUB)
            pivot = jnp.broadcast_to(cols[j][gj][sj : sj + 1], (SUB, LANES))
            diagonal[gj] = jnp.where(row_id == sj, pivot, diagonal[gj])
            inverse = 1.0 / pivot
            below = {g: cols[j][g] for g in range(gj, groups)}
            below[gj] = jnp.where(row_id > sj, below[gj], 0.0)
            factor = {g: below[g] * inverse for g in range(gj, groups)}
            for k in range(j + 1, p + panel):
                row = jnp.broadcast_to(cols[k][gj][sj : sj + 1], (SUB, LANES))
                for g in range(gj, groups):
                    if k == j + 1:
                        cols[k][g] = cols[k][g] - (below[g] * row) * inverse
                    else:
                        cols[k][g] = cols[k][g] - factor[g] * row
            for h in range(2):
                source = tiles[gj][h][sj : sj + 1]
                if h == half:
                    source = jnp.where(lane_id[0:1] == lane0 + j, 1.0, source)
                row = jnp.broadcast_to(source, (SUB, LANES))
                for g in range(gj, groups):
                    tile = tiles[g][h]
                    if h == half:
                        tile = jnp.where((lane_id == lane0 + j) & ((row_id > sj) if g == gj else True), 0.0, tile)
                    tiles[g][h] = tile - factor[g] * row
                if h == half:
                    tiles[gj][h] = jnp.where((lane_id == lane0 + j) & (row_id == sj), 1.0, tiles[gj][h])
    out = []
    for g in range(groups):
        r = lax.rsqrt(diagonal[g])
        r = r * (1.5 - 0.5 * diagonal[g] * r * r)
        above = (lane_id > lane0 + g * SUB + row_id) & (lane_id < lane0 + BLOCK)
        tiles[g][half] = jnp.where(above, 0.0, tiles[g][half])
        out.append([tiles[g][h] * r for h in range(2)])
    return out


def factor(work, inverse, visit):
    n = work.shape[0]
    col_id = lax.broadcasted_iota(jnp.int32, (BLOCK, n), 1)
    for start in range(0, n, BLOCK):
        strip = [
            [work[start + SUB * g : start + SUB * (g + 1), LANES * h : LANES * (h + 1)] for h in range(2)]
            for g in range(BLOCK // SUB)
        ]
        done = eliminate(strip, start)
        rows = jnp.concatenate([jnp.concatenate(t, axis=1) for t in done], axis=0)
        inverse[start : start + BLOCK, :] = jnp.where(col_id < start + BLOCK, rows, 0.0)
        after = start + BLOCK
        visit(start, after)
        for lo, hi in ((after, after + BLOCK), (after + BLOCK, n)):
            if lo >= n or lo >= hi:
                continue
            base = work[lo:hi, :]
            ids = lax.broadcasted_iota(jnp.int32, (hi - lo, n), 1)
            base = jnp.where((ids >= start) & (ids < after), 0.0, base)
            step = dot(rows[:, lo:hi], rows, ((0,), (0,)), EXACT)
            work[lo:hi, :] = base - step


def dot(left, right, contract, precision=None):
    return lax.dot_general(
        left, right, (contract, ((), ())), precision=precision, preferred_element_type=F32
    )


def split(value):
    high = value.astype(jnp.bfloat16)
    return high, (value - high.astype(F32)).astype(jnp.bfloat16)


NN = ((1,), (0,))


def split_dot(left, right):
    return dot(left[0], right[0], NN) + (dot(left[0], right[1], NN) + dot(left[1], right[0], NN))


def prepare_kernel(matrix, high, low):
    high[...], low[...] = split(matrix[...])


def pick_kernel(place, *refs):
    sources, out, done = refs[:-2], refs[-2], refs[-1]
    for z in range(4):

        @pl.when(place[2] == z)
        def _():
            copies = []
            begin = 0
            for source in sources[2 * z : 2 * z + 2]:
                step = source.shape[0] // 4
                for i in range(4):
                    copies.append(
                        pltpu.make_async_copy(
                            source.at[i * step : (i + 1) * step],
                            out.at[begin + i * step : begin + (i + 1) * step],
                            done.at[len(copies)],
                        )
                    )
                begin += source.shape[0]
            for copy in copies:
                copy.start()
            for copy in copies:
                copy.wait()


def product_kernel(place, panel_here, panel_sent, upper_pieces, upper_rest, lower_pieces, lower_rest, out, panel_high, panel_low):
    half, cols = upper_pieces.shape
    sent = place[3] == 1
    for start, matrix_high, matrix_low in ((0, upper_pieces, upper_rest), (half, lower_pieces, lower_rest)):
        part = slice(start, start + half)
        panel = jnp.where(sent, panel_sent[part], panel_here[part])
        first, second = split(panel)
        third = ((panel - first.astype(F32)) - second.astype(F32)).astype(jnp.bfloat16)
        panel_high[part] = first
        panel_low[part] = second
        pieces = split(panel.T)
        for c in range(0, cols, PANEL):
            here = slice(c, c + PANEL)
            value = split_dot(pieces, (matrix_high[:, here], matrix_low[:, here]))
            out[:, here] = value if start == 0 else out[:, here] + value
        cross = dot(pieces[0], second, NN) + dot(pieces[0], third, NN)
        value = dot(pieces[0], first, NN) + (dot(pieces[1], second, NN) + (cross + cross.T))
        out[:, cols:] = value if start == 0 else out[:, cols:] + value


def finish_kernel(place, gathered, panel_high, panel_low, matrix, upper, out, work, inverse, found, first, second, coeff, coeff_low, held, arrived, left):
    blocks = matrix.shape[0] // ROWS
    cols = matrix.shape[1]
    scale = float(matrix.shape[0] * (PANEL // upper.shape[0])) ** 0.5

    def fetch(b):
        part = slice(b * ROWS, b * ROWS + ROWS)
        return pltpu.make_async_copy(matrix.at[part], held.at[part], arrived.at[b])

    def send(b):
        part = slice(b * ROWS, b * ROWS + ROWS)
        return pltpu.make_async_copy(held.at[part], out.at[part], left.at[b])

    for b in range(blocks):
        fetch(b).start()
    holds = place[0] == 1
    work[...] = gathered[:, cols:]
    first[...], second[...] = split(gathered[:, :cols])

    def visit(start, after):
        depth = -(-after // LANES) * LANES
        rows = split(inverse[start:after, :depth])
        found[start:after, :] = split_dot(rows, (first[:depth, :], second[:depth, :]))

    factor(work, inverse, visit)
    turned = inverse[...].T
    upward = split(turned)
    height = upper.shape[0]
    mine = pl.ds(pl.multiple_of(place[1] * height, height), height)
    for c in range(0, cols, PANEL):
        here = slice(c, c + PANEL)
        weights = split_dot(upward, split(found[:, here]))
        if c == 0:
            weights = jnp.where(holds, -scale * turned, weights)
        coeff[:, here], coeff_low[:, here] = split(weights)
    upper[...] = found[mine, :]

    for b in range(blocks):
        part = slice(b * ROWS, b * ROWS + ROWS)
        fetch(b).wait()
        panel = (panel_high[part], panel_low[part])
        for c in range(0, cols, PANEL):
            here = slice(c, c + PANEL)
            change = split_dot(panel, (coeff[:, here], coeff_low[:, here]))
            value = held[part, here]
            if c == 0:
                value = jnp.where(holds, 0.0, value)
            held[part, here] = value - change
        send(b).start()
    for b in range(blocks):
        send(b).wait()


VMEM = pl.BlockSpec(memory_space=pltpu.VMEM)
SMEM = pl.BlockSpec(memory_space=pltpu.SMEM)
HBM = pl.BlockSpec(memory_space=pltpu.HBM)


def prepare(matrix, part=0, parts=1):
    count = 2 * matrix.shape[0] // ROWS // parts
    shape = jax.ShapeDtypeStruct((matrix.shape[0] // parts, matrix.shape[1]), jnp.bfloat16)
    block = pl.BlockSpec((ROWS // 2, matrix.shape[1]), lambda i: (i, 0))
    return pl.pallas_call(
        prepare_kernel,
        grid=(count,),
        out_shape=(shape, shape),
        in_specs=[pl.BlockSpec((ROWS // 2, matrix.shape[1]), lambda i: (i + part * count, 0))],
        out_specs=(block, block),
        compiler_params=pltpu.CompilerParams(vmem_limit_bytes=12 << 20),
        cost_estimate=pl.CostEstimate(flops=2 * 10**9, bytes_accessed=8 << 20, transcendentals=0),
    )(matrix)


def pick(place, sources):
    low, width = sources[0].shape
    high = sources[1].shape[0]
    return pl.pallas_call(
        pick_kernel,
        out_shape=jax.ShapeDtypeStruct((low + high, width), F32),
        in_specs=[SMEM] + [HBM] * len(sources),
        out_specs=VMEM,
        scratch_shapes=[pltpu.SemaphoreType.DMA((8,))],
        compiler_params=pltpu.CompilerParams(vmem_limit_bytes=8 << 20),
        cost_estimate=pl.CostEstimate(flops=10**8, bytes_accessed=4 << 20, transcendentals=0),
    )(place, *sources)


def products(place, panel_here, panel_sent, pieces):
    rows, cols = panel_here.shape[0], pieces[0].shape[1]
    narrow = jax.ShapeDtypeStruct((rows, PANEL), jnp.bfloat16)
    return pl.pallas_call(
        product_kernel,
        out_shape=(jax.ShapeDtypeStruct((PANEL, cols + PANEL), F32), narrow, narrow),
        in_specs=[SMEM] + [VMEM] * 6,
        out_specs=[VMEM] * 3,
        compiler_params=pltpu.CompilerParams(vmem_limit_bytes=32 << 20),
        cost_estimate=pl.CostEstimate(flops=5 * 10**9, bytes_accessed=16 << 20, transcendentals=0),
    )(place, panel_here, panel_sent, *pieces)


def finish(place, gathered, panel_high, panel_low, matrix, height):
    rows, cols = matrix.shape
    return pl.pallas_call(
        finish_kernel,
        out_shape=(
            jax.ShapeDtypeStruct((height, cols), F32),
            jax.ShapeDtypeStruct(matrix.shape, F32),
        ),
        in_specs=[SMEM] + [VMEM] * 3 + [HBM],
        out_specs=[VMEM, HBM],
        scratch_shapes=[
            pltpu.VMEM((PANEL, PANEL), F32),
            pltpu.VMEM((PANEL, PANEL), F32),
            pltpu.VMEM((PANEL, cols), F32),
            pltpu.VMEM((PANEL, cols), jnp.bfloat16),
            pltpu.VMEM((PANEL, cols), jnp.bfloat16),
            pltpu.VMEM((PANEL, cols), jnp.bfloat16),
            pltpu.VMEM((PANEL, cols), jnp.bfloat16),
            pltpu.VMEM(matrix.shape, F32),
            pltpu.SemaphoreType.DMA((rows // ROWS,)),
            pltpu.SemaphoreType.DMA((rows // ROWS,)),
        ],
        compiler_params=pltpu.CompilerParams(vmem_limit_bytes=50 << 20),
        cost_estimate=pl.CostEstimate(flops=8 * 10**9, bytes_accessed=24 << 20, transcendentals=0),
    )(place, gathered, panel_high, panel_low, matrix)


def total_kernel(tiles, out):
    total = tiles[0]
    for i in range(1, tiles.shape[0]):
        total = total + tiles[i]
    for i in range(out.shape[0]):
        out[i] = total


def exchange(tiles):
    return lax.all_to_all(tiles, "row", 0, 0, tiled=True)


def sum_everywhere(value):
    count = lax.axis_size("row")
    tiles = exchange(value.reshape(count, value.shape[0] // count, value.shape[1]))
    copies = pl.pallas_call(
        total_kernel,
        out_shape=jax.ShapeDtypeStruct(tiles.shape, F32),
        in_specs=[VMEM],
        out_specs=VMEM,
        compiler_params=pltpu.CompilerParams(vmem_limit_bytes=8 << 20),
        cost_estimate=pl.CostEstimate(flops=10**7, bytes_accessed=3 << 20, transcendentals=0),
    )(tiles)
    return exchange(copies).reshape(value.shape)


def shards(matrix):
    col = lax.axis_index(COL)
    place = jnp.stack([col == 0, lax.axis_index("row"), col // 2, col % 2]).astype(jnp.int32)
    half = matrix.shape[0] * 35 // 64
    own_low = lax.optimization_barrier(matrix[:half, :PANEL])
    own_high = lax.optimization_barrier(matrix[half:, :PANEL])
    first_low = lax.ppermute(own_low, COL, [(0, 2)])
    first_high = lax.ppermute(own_high, COL, [(0, 6)])
    second_low = lax.ppermute(own_low, COL, [(0, 6)])
    second_high = lax.ppermute(own_high, COL, [(0, 2)])
    pieces = prepare(matrix, 0, 2)
    pieces += prepare(matrix, 1, 2)
    relay_low = lax.ppermute(first_low, COL, [(2, 4)])
    relay_high = lax.ppermute(first_high, COL, [(6, 4)])
    here = pick(place, (own_low, own_high, first_low, second_high, relay_low, relay_high, second_low, first_high))
    sent = lax.ppermute(here, COL, [(0, 1), (2, 3), (4, 5), (6, 7)])
    product, panel_high, panel_low = products(place, here, sent, pieces)
    gathered = sum_everywhere(product)
    height = PANEL // lax.axis_size("row")
    upper, reduced = finish(place, gathered, panel_high, panel_low, matrix, height)
    return (upper, reduced)


def solution(mesh):
    finer = Mesh(mesh.devices.reshape(mesh.shape["row"], 4, 2), ("row", *COL))
    return jax.shard_map(
        shards,
        mesh=finer,
        in_specs=(P("row", COL),),
        out_specs=(P("row", COL), P("row", COL)),
        check_vma=False,
    )
```
